32 devices in a mesh: node: 4 (over z), slab: 8 (over y, x, core).
Axes of the slice: x: 2, y: 2, z: 4, core: 2. Of those that a mesh axis runs over, the one named last changes fastest.
Arguments:
- initial: float32 [32, 256, 256], P('slab'), may hold values from -20 to 20
- sections: float32 [4, 32, 256, 256], P('node', 'slab'), may hold values from -21 to 21
Outputs:
- new_sections: float32 [4, 32, 256, 256], P('node', 'slab')
- residual_max: float32 [3], replicated
The draws below stay inside these ranges and needn't reach their ends.
All inputs are finite; a program needn't handle non-finite values.
Results may differ from the reference program's by a relative error of at most 0.0003.
Values sent between devices are 32-bit elements; how exact they have to be, the bound alone decides.
A program may use at most 64 MiB of HBM per device.

```python
import math
import jax
import jax.numpy as jnp
from jax import lax

M = 4
SWEEPS = 3
NY = 256
NZ = 256
NX = 32


def base_field(key):
    grid_shape = (NX, NY, NZ)
    position = jnp.arange(NX).astype(jnp.float32) / NX
    plane_scale = 10.0 ** (position - 0.5)
    factors = jax.random.uniform(jax.random.fold_in(key, 1), grid_shape, jnp.float32, 0.5, 1.5)
    values = jax.random.truncated_normal(jax.random.fold_in(key, 2), -4.0, 4.0, grid_shape, jnp.float32)
    return values * factors * plane_scale[:, None, None]


def draw_initial(key, part):
    return base_field(key)


def draw_sections(key, part):
    perturb = jax.random.truncated_normal(jax.random.fold_in(key, 3), -4.0, 4.0, (M, NX, NY, NZ), jnp.float32)
    return base_field(key)[None] + 0.2 * perturb


def setup_inputs(seed: int = 0) -> dict:
    seeds = jax.random.split(jax.random.key(seed), 3)
    initial = draw_initial(jax.random.fold_in(seeds[2], 71), 0)
    sections = draw_sections(jax.random.fold_in(seeds[2], 71), 0)
    return {"initial": initial, "sections": sections}


diffusion_step = 4.0


def radau_value(order, point):
    prev_value = 1.0
    prev_slope = 0.0
    this_value = point
    this_slope = 1.0
    for degree in range(1, order):
        next_value = ((2 * degree + 1) * point * this_value - degree * prev_value) / (degree + 1)
        next_slope = ((2 * degree + 1) * (this_value + point * this_slope) - degree * prev_slope) / (degree + 1)
        prev_value, prev_slope = this_value, this_slope
        this_value, this_slope = next_value, next_slope
    return this_value - prev_value, this_slope - prev_slope


def radau_tables(node_total):
    points = []
    for node_index in range(node_total):
        estimate = math.cos(2.0 * math.pi * node_index / (2 * node_total - 1))
        if node_index > 0:
            for repeat in range(60):
                poly_value, poly_slope = radau_value(node_total, estimate)
                estimate = estimate - poly_value / poly_slope
        points.append((estimate + 1.0) / 2.0)
    points = sorted(points)
    quadrature = []
    for row_index in range(node_total):
        entries = []
        for column_index in range(node_total):
            coeffs = [1.0]
            for other_index in range(node_total):
                if other_index != column_index:
                    divisor = points[column_index] - points[other_index]
                    shifted = [0.0] + coeffs
                    widened = coeffs + [0.0]
                    coeffs = [(shifted[place] - points[other_index] * widened[place]) / divisor for place in range(len(shifted))]
            integral = 0.0
            for place in range(len(coeffs)):
                integral = integral + coeffs[place] * points[row_index] ** (place + 1) / (place + 1)
            entries.append(integral)
        quadrature.append(entries)
    return points, quadrature


def laplacian(grid_values):
    beside = jnp.roll(grid_values, 1, 0) + jnp.roll(grid_values, -1, 0)
    beside = beside + jnp.roll(grid_values, 1, 1) + jnp.roll(grid_values, -1, 1)
    beside = beside + jnp.roll(grid_values, 1, 2) + jnp.roll(grid_values, -1, 2)
    return beside - 6.0 * grid_values


def eigen_line(length):
    indices = jnp.arange(length).astype(jnp.float32)
    return 2.0 * jnp.cos(indices * (2.0 * math.pi / length)) - 2.0


def reference(initial, sections):
    nodes_list, quad_list = radau_tables(M)
    nodes_at = jnp.asarray(nodes_list, jnp.float32)
    quadrature = jnp.asarray(quad_list, jnp.float32)
    spectrum = eigen_line(NX)[:, None, None] + eigen_line(NY)[None, :, None] + eigen_line(NZ)[None, None, :]
    current = sections
    maxima = []
    for sweep_index in range(SWEEPS):
        slopes = lax.map(laplacian, current)
        combined = jnp.einsum("mj,jxyz->mxyz", quadrature, slopes, precision=lax.Precision.HIGHEST)
        residual = initial[None] + diffusion_step * combined - current
        maxima.append(jnp.max(jnp.abs(residual)))
        diagonal = nodes_at / (sweep_index + 1.0)
        right_side = initial[None] + diffusion_step * (combined - diagonal[:, None, None, None] * slopes)

        def solve_one(pair):
            grid_values, weight = pair
            transformed = jnp.fft.fftn(grid_values)
            solved = jnp.fft.ifftn(transformed / (1.0 - diffusion_step * weight * spectrum))
            return jnp.real(solved).astype(jnp.float32)

        current = lax.map(solve_one, (right_side, diagonal))
    return current, jnp.stack(maxima)
```

```python
import math

import jax
import jax.numpy as jnp
from jax import lax
from jax.sharding import PartitionSpec as P

SWEEPS = 3


diffusion_step = 4.0
high = lax.Precision.HIGH


def radau_value(order, point):
    prev_value = 1.0
    prev_slope = 0.0
    this_value = point
    this_slope = 1.0
    for degree in range(1, order):
        next_value = ((2 * degree + 1) * point * this_value - degree * prev_value) / (degree + 1)
        next_slope = (
            (2 * degree + 1) * (this_value + point * this_slope) - degree * prev_slope
        ) / (degree + 1)
        prev_value, prev_slope = (this_value, this_slope)
        this_value, this_slope = (next_value, next_slope)
    return (this_value - prev_value, this_slope - prev_slope)


def radau_tables(node_total):
    points = []
    for node_index in range(node_total):
        estimate = math.cos(2.0 * math.pi * node_index / (2 * node_total - 1))
        if node_index > 0:
            for repeat in range(60):
                poly_value, poly_slope = radau_value(node_total, estimate)
                estimate = estimate - poly_value / poly_slope
        points.append((estimate + 1.0) / 2.0)
    points = sorted(points)
    quadrature = []
    for row_index in range(node_total):
        entries = []
        for column_index in range(node_total):
            coeffs = [1.0]
            for other_index in range(node_total):
                if other_index != column_index:
                    divisor = points[column_index] - points[other_index]
                    shifted = [0.0] + coeffs
                    widened = coeffs + [0.0]
                    coeffs = [
                        (shifted[place] - points[other_index] * widened[place]) / divisor
                        for place in range(len(shifted))
                    ]
            integral = 0.0
            for place in range(len(coeffs)):
                integral = integral + coeffs[place] * points[row_index] ** (place + 1) / (place + 1)
            entries.append(integral)
        quadrature.append(entries)
    return (points, quadrature)


def cas_table(length):
    indices = lax.iota(jnp.int32, length)
    products = indices[:, None] * indices[None, :] % length
    phases = products.astype(jnp.float32) * (2.0 * math.pi / length)
    return jnp.cos(phases) + jnp.sin(phases)


def eigen_line(length):
    indices = lax.iota(jnp.int32, length).astype(jnp.float32)
    return 2.0 * jnp.cos(indices * (2.0 * math.pi / length)) - 2.0


def on_device(initial, sections):
    node_count = lax.axis_size("node")
    slab_count = lax.axis_size("slab")
    both = ("node", "slab")
    total_count = node_count * slab_count
    slab_cells, cells_y, cells_z = initial.shape
    total_x = slab_cells * slab_count
    share = max(slab_cells // node_count, 1)
    repeats = max(node_count // slab_cells, 1)
    rows = cells_y // total_count
    scale_back = 1.0 / float(total_x * cells_y * cells_z)
    nodes_list, quad_list = radau_tables(node_count)
    my_node = lax.axis_index("node")
    my_place = my_node * slab_count + lax.axis_index("slab")
    cas_x = cas_table(total_x)
    cas_y = cas_table(cells_y)
    cas_z = cas_table(cells_z)
    eigen_y = lax.dynamic_slice_in_dim(eigen_line(cells_y), my_place * rows, rows, 0)
    spectrum = (
        eigen_line(total_x)[:, None, None]
        + eigen_y[None, :, None]
        + eigen_line(cells_z)[None, None, :]
    )
    mine = lax.dynamic_slice_in_dim(initial, my_node // repeats * share, share, 0)
    planes = jnp.concatenate([sections[0], mine], axis=0)
    planes = jnp.einsum("cyz,yv->cvz", planes, cas_y, precision=high)
    pencils = lax.all_to_all(planes, both, split_axis=1, concat_axis=0, tiled=True)
    pencils = jnp.einsum("cyz,zw->cyw", pencils, cas_z, precision=high)
    pencils = pencils.reshape(node_count, slab_count, slab_cells + share, rows, cells_z)
    iterate = jnp.einsum(
        "nsiyw,sia->nayw",
        pencils[:, :, :slab_cells],
        cas_x.reshape(slab_count, slab_cells, total_x),
        precision=high,
    )
    start = jnp.einsum(
        "nsiyw,snia->ayw",
        pencils[::repeats, :, slab_cells:],
        cas_x.reshape(slab_count, node_count // repeats, share, total_x),
        precision=high,
    )
    values = [iterate[m] for m in range(node_count)]
    stretched = diffusion_step * spectrum
    residuals = []
    for m in range(node_count):
        mixed = sum(quad_list[m][j] * values[j] for j in range(node_count))
        residuals.append(start + stretched * mixed - values[m])
    fields = [jnp.stack(residuals)]
    for sweep_index in range(SWEEPS):
        change = []
        for m in range(node_count):
            weight = nodes_list[m] / (sweep_index + 1.0)
            change.append(residuals[m] / (1.0 - weight * stretched))
        values = [values[m] + change[m] for m in range(node_count)]
        if sweep_index + 1 < SWEEPS:
            slopes = [stretched * change[m] for m in range(node_count)]
            residuals = [
                residuals[m]
                - change[m]
                + sum(quad_list[m][j] * slopes[j] for j in range(node_count))
                for m in range(node_count)
            ]
            fields.append(jnp.stack(residuals))
    fields.append(jnp.stack(values))
    fields = jnp.stack(fields)
    back_x = cas_x.reshape(total_x, slab_count, slab_cells) * scale_back
    outward = jnp.einsum("fmayw,asi->msfiyw", fields, back_x, precision=high)
    outward = jnp.einsum("msfiyw,wz->msfiyz", outward, cas_z, precision=high)
    outward = outward.reshape(-1, rows, cells_z)
    arrived = lax.all_to_all(outward, both, split_axis=0, concat_axis=1, tiled=True)
    arrived = jnp.einsum("cyz,yv->cvz", arrived, cas_y, precision=high)
    arrived = arrived.reshape(SWEEPS + 1, slab_cells, cells_y, cells_z)
    largest = jnp.max(jnp.abs(arrived[:SWEEPS]), axis=(1, 2, 3))
    spread = jnp.broadcast_to(largest[None], (total_count, SWEEPS))
    result = jnp.max(
        lax.all_to_all(spread, both, split_axis=0, concat_axis=0, tiled=True), axis=0
    )
    return (arrived[SWEEPS:], result)


def solution(mesh):
    placed = (P("slab", None, None), P("node", "slab", None, None))
    return jax.shard_map(
        on_device,
        mesh=mesh,
        in_specs=placed,
        out_specs=(P("node", "slab", None, None), P()),
        check_vma=False,
    )
```

```python
import functools
import math

import jax
import jax.numpy as jnp
from jax import lax
from jax.experimental import pallas as pl
from jax.experimental.pallas import tpu as pltpu
from jax.sharding import PartitionSpec as P

SWEEPS = 3


diffusion_step = 4.0
MESH = pl.DeviceIdType.MESH


def radau_value(order, point):
    prev_value = 1.0
    prev_slope = 0.0
    this_value = point
    this_slope = 1.0
    for degree in range(1, order):
        next_value = ((2 * degree + 1) * point * this_value - degree * prev_value) / (degree + 1)
        next_slope = (
            (2 * degree + 1) * (this_value + point * this_slope) - degree * prev_slope
        ) / (degree + 1)
        prev_value, prev_slope = (this_value, this_slope)
        this_value, this_slope = (next_value, next_slope)
    return (this_value - prev_value, this_slope - prev_slope)


def radau_tables(node_total):
    points = []
    for node_index in range(node_total):
        estimate = math.cos(2.0 * math.pi * node_index / (2 * node_total - 1))
        if node_index > 0:
            for repeat in range(60):
                poly_value, poly_slope = radau_value(node_total, estimate)
                estimate = estimate - poly_value / poly_slope
        points.append((estimate + 1.0) / 2.0)
    points = sorted(points)
    quadrature = []
    for row_index in range(node_total):
        entries = []
        for column_index in range(node_total):
            coeffs = [1.0]
            for other_index in range(node_total):
                if other_index != column_index:
                    divisor = points[column_index] - points[other_index]
                    shifted = [0.0] + coeffs
                    widened = coeffs + [0.0]
                    coeffs = [
                        (shifted[place] - points[other_index] * widened[place]) / divisor
                        for place in range(len(shifted))
                    ]
            integral = 0.0
            for place in range(len(coeffs)):
                integral = integral + coeffs[place] * points[row_index] ** (place + 1) / (place + 1)
            entries.append(integral)
        quadrature.append(entries)
    return (points, quadrature)


def cas_table(length):
    indices = lax.iota(jnp.int32, length)
    products = indices[:, None] * indices[None, :] % length
    phases = products.astype(jnp.float32) * (2.0 * math.pi / length)
    return jnp.cos(phases) + jnp.sin(phases)


def eigen_line(length):
    indices = lax.iota(jnp.int32, length).astype(jnp.float32)
    return 2.0 * jnp.cos(indices * (2.0 * math.pi / length)) - 2.0


def split_terms(value):
    upper = value.astype(jnp.bfloat16)
    lower = (value - upper.astype(jnp.float32)).astype(jnp.bfloat16)
    return upper, lower


def table_terms(table):
    upper = lax.reduce_precision(table, 8, 7)
    return jnp.stack([upper.astype(jnp.bfloat16), (table - upper).astype(jnp.bfloat16)])


def product(left, right):
    def one(a, b):
        return jnp.dot(a, b, preferred_element_type=jnp.float32)

    return one(left[0], right[0]) + (one(left[0], right[1]) + one(left[1], right[0]))


def loop(count, step, carry, group=4):
    group = group if count % group == 0 else 1

    def body(index, state):
        for offset in range(group):
            state = step(index * group + offset, state)
        return state

    return lax.fori_loop(0, count // group, body, carry)


def sweeps_kernel(
    nodes, quad, u, first, lam, ymat_ref, zmat_ref, out, top,
    planes, gathered, start, resid, front, outward, arrived, rho, gain, close, peak, peers, lines,
    send_u, recv_u, send_i, recv_i, send_z, recv_z, send_r, recv_r, send_m, recv_m, local,
):
    node_count, slab_count = len(nodes), lax.axis_size("slab")
    me, here = lax.axis_index("node"), lax.axis_index("slab")
    cells, size_y, size_z = u.shape
    chunks, total_x, rows = gathered.shape[0], gathered.shape[2], gathered.shape[3]
    band = chunks * rows
    scale = 1.0 / float(size_y * size_z)

    def other_slab(step):
        return lax.rem(here + step, slab_count)

    def other_node(step):
        return lax.rem(me + step, node_count)

    def to(src, dst, send, recv, node, slab):
        return pltpu.make_async_remote_copy(
            src_ref=src, dst_ref=dst, send_sem=send, recv_sem=recv,
            device_id=(node, slab), device_id_type=MESH,
        )

    barrier = pltpu.get_barrier_semaphore()
    for step in range(1, slab_count):
        pl.semaphore_signal(barrier, inc=1, device_id=(me, other_slab(step)), device_id_type=MESH)
    for step in range(1, node_count):
        pl.semaphore_signal(barrier, inc=1, device_id=(other_node(step), here), device_id_type=MESH)

    def transform(value):
        part = product(split_terms(value), (zmat_ref[0], zmat_ref[1]))
        return product((ymat_ref[0], ymat_ref[1]), split_terms(part))

    def source(field, chunk, slab):
        return planes.at[field, :, pl.ds(slab * band + chunk * rows, rows), :]

    def target(field, chunk, slab):
        span = pl.ds(slab * cells, cells)
        return gathered.at[chunk, me, span] if field == 0 else start.at[chunk, span]

    def send_field(field, send, recv):
        for chunk in range(chunks):
            pltpu.make_async_copy(
                source(field, chunk, here), target(field, chunk, here), local.at[field, chunk]
            ).start()
            for step in range(1, slab_count):
                slab = other_slab(step)
                to(
                    source(field, chunk, slab), target(field, chunk, here),
                    send.at[chunk, step], recv.at[chunk, step], me, slab,
                ).start()

    def take_field(field, chunk, send, recv):
        pltpu.make_async_copy(
            source(field, chunk, here), target(field, chunk, here), local.at[field, chunk]
        ).wait()
        for step in range(1, slab_count):
            slab = lax.rem(here + slab_count - step, slab_count)
            to(
                source(field, chunk, slab), target(field, chunk, slab),
                send.at[chunk, step], recv.at[chunk, step], me, slab,
            ).wait()

    def enter(index, state):
        planes[0, index] = transform(u[index])
        return state

    def enter_first(index, state):
        planes[1, index] = transform(first[index])
        return state

    lax.fori_loop(0, cells, enter, 0)
    pl.semaphore_wait(barrier, slab_count - 1 + node_count - 1)
    send_field(0, send_u, recv_u)
    lax.fori_loop(0, cells, enter_first, 0)
    send_field(1, send_i, recv_i)

    def piece(chunk, origin, direction):
        target_node = me + 1 if direction == 0 else me - 1
        slot = gathered.at[chunk, origin]
        return to(
            slot, slot, send_z.at[chunk, origin, direction], recv_z.at[chunk, origin],
            target_node, here,
        )

    has_right, has_left = me < node_count - 1, me > 0

    for chunk in range(chunks):
        take_field(0, chunk, send_u, recv_u)

        @pl.when(has_right)
        def _():
            piece(chunk, me, 0).start()

        @pl.when(has_left)
        def _():
            piece(chunk, me, 1).start()

    def relay(chunk):
        for away in range(1, node_count):

            @pl.when(me - away >= 0)
            def _():
                piece(chunk, me - away, 0).wait_recv()

                @pl.when(has_right)
                def _():
                    piece(chunk, me - away, 0).start()

            @pl.when(me + away < node_count)
            def _():
                piece(chunk, me + away, 1).wait_recv()

                @pl.when(has_left)
                def _():
                    piece(chunk, me + away, 1).start()

    def mix(table, values):
        mixed = []
        for line in table:
            total = line[0] * values[0]
            for weight, value in zip(line[1:], values[1:]):
                total = total + weight * value
            mixed.append(total)
        return mixed

    def solve(chunk):
        eigen = lam[pl.ds(chunk * rows, rows), :]

        def blend(x, state):
            values = [gathered[chunk, j, x] for j in range(node_count)]
            for m, value in enumerate(mix(quad, values)):
                front[x, m] = value
            return state

        def begin(x, state):
            below = lax.rem(x + total_x - 1, total_x)
            above = lax.rem(x + 1, total_x)
            for m in range(node_count):
                slope = front[below, m] + front[above, m] + (eigen - 2.0) * front[x, m]
                resid[x, m] = start[chunk, x] + diffusion_step * slope - gathered[chunk, m, x]
            return state

        loop(total_x, blend, 0)
        loop(total_x, begin, 0)
        for sweep in range(SWEEPS):
            last = sweep + 1 == SWEEPS
            for m in range(node_count):
                reach = diffusion_step * nodes[m] / (sweep + 1.0)
                excess = 1.0 / reach - eigen
                root = jnp.sqrt(excess * (excess + 4.0))
                ratio = 2.0 / (excess + 2.0 + root)
                rho[m] = ratio
                gain[m] = 1.0 / (reach * root)
                power, base, left = None, ratio, total_x
                while left:
                    if left % 2:
                        power = base if power is None else power * base
                    base, left = base * base, left // 2
                close[m] = 1.0 / (1.0 - power)
            pick = pl.ds(me, 1) if last else pl.ds(0, node_count)
            width = 1 if last else node_count
            ratio = rho[pick]
            factor = gain[pick]

            def gather_ends(x, state):
                up, down = state
                return (resid[x, pick] + ratio * up, resid[total_x - 1 - x, pick] + ratio * down)

            zero = jnp.zeros((width, rows, size_z), jnp.float32)
            up, down = loop(total_x, gather_ends, (zero, zero))
            closing = close[pick]

            def forward(x, state):
                state = resid[x, pick] + ratio * state
                front[x, pick] = state
                outward[chunk, sweep, x] = resid[x, me]
                return state

            def backward(index, state):
                x = total_x - 1 - index
                held = resid[x, pick]
                beyond = ratio * state
                change = factor * (front[x, pick] + beyond)
                front[x, pick] = change
                if sweep == 0:
                    outward[chunk, SWEEPS, x] = front[x, me]
                else:
                    outward[chunk, SWEEPS, x] = outward[chunk, SWEEPS, x] + front[x, me]
                if not last:
                    moved = change - held
                    table = [
                        [quad[m][j] * (sweep + 1.0) / nodes[j] - (1.0 if m == j else 0.0)
                         for j in range(node_count)]
                        for m in range(node_count)
                    ]
                    for m, value in enumerate(mix(table, [moved[j] for j in range(node_count)])):
                        resid[x, m] = value
                return held + beyond

            loop(total_x, forward, up * closing)
            loop(total_x, backward, down * closing, 2)

    def back_source(chunk, slab):
        return outward.at[chunk, :, pl.ds(slab * cells, cells)]

    def back_target(chunk, slab):
        return arrived.at[:, :, pl.ds(slab * band + chunk * rows, rows), :]

    for chunk in range(chunks):
        relay(chunk)
        take_field(1, chunk, send_i, recv_i)
        solve(chunk)
        pltpu.make_async_copy(
            back_source(chunk, here), back_target(chunk, here), local.at[2, chunk]
        ).start()
        for step in range(1, slab_count):
            slab = other_slab(step)
            to(
                back_source(chunk, slab), back_target(chunk, here),
                send_r.at[chunk, step], recv_r.at[chunk, step], me, slab,
            ).start()
    for chunk in range(chunks):
        pltpu.make_async_copy(
            back_source(chunk, here), back_target(chunk, here), local.at[2, chunk]
        ).wait()
        for step in range(1, slab_count):
            slab = lax.rem(here + slab_count - step, slab_count)
            to(
                back_source(chunk, slab), back_target(chunk, slab),
                send_r.at[chunk, step], recv_r.at[chunk, step], me, slab,
            ).wait()
        for origin in range(node_count):

            @pl.when(jnp.logical_and(has_right, origin <= me))
            def _():
                piece(chunk, origin, 0).wait_send()

            @pl.when(jnp.logical_and(has_left, origin >= me))
            def _():
                piece(chunk, origin, 1).wait_send()

    peak[...] = jnp.zeros_like(peak)
    for sweep in range(SWEEPS):

        def finish(index, state):
            value = jnp.abs(transform(arrived[sweep, index]))
            return jnp.maximum(state, jnp.max(value.reshape(-1, 8, size_z), axis=0))

        most = lax.fori_loop(0, cells, finish, jnp.zeros((8, size_z), jnp.float32))
        most = jnp.max(jnp.max(most, axis=1, keepdims=True), axis=0, keepdims=True) * scale
        peak[sweep : sweep + 1, :] = jnp.broadcast_to(most, (1, peak.shape[1]))

    def swap(count, slots, level, place):
        for step in range(1, count):
            to(peak, slots.at[step], send_m.at[level, step], recv_m.at[level, step], *place(step)).start()

    def settle(count, slots, level, place):
        for step in range(1, count):
            to(peak, slots.at[step], send_m.at[level, step], recv_m.at[level, step], *place(step)).wait()
        best = peak[...]
        for step in range(1, count):
            best = jnp.maximum(best, slots[step])
        return best

    def along_slab(step):
        return (me, other_slab(step))

    def along_node(step):
        return (other_node(step), here)

    def leave(index, state):
        out[index] = u[index] + scale * transform(arrived[SWEEPS, index])
        return state

    swap(slab_count, peers, 0, along_slab)
    lax.fori_loop(0, cells // 2, leave, 0)
    peak[...] = settle(slab_count, peers, 0, along_slab)
    swap(node_count, lines, 1, along_node)
    lax.fori_loop(cells // 2, cells, leave, 0)
    top[...] = settle(node_count, lines, 1, along_node)


def on_device(initial, sections):
    node_count = lax.axis_size("node")
    slab_count = lax.axis_size("slab")
    cells, size_y, size_z = initial.shape
    total_x = cells * slab_count
    nodes, quad = radau_tables(node_count)
    band = size_y // slab_count
    rows = 8
    chunks = band // rows
    eigen_y = lax.dynamic_slice_in_dim(
        eigen_line(size_y), lax.axis_index("slab") * band, band, 0
    )
    lam = eigen_y[:, None] + eigen_line(size_z)[None, :]
    matrix_y = table_terms(cas_table(size_y))
    matrix_z = table_terms(cas_table(size_z))
    whole = pl.BlockSpec(memory_space=pltpu.VMEM)

    def room(*shape):
        return pltpu.VMEM(shape, jnp.float32)

    dma = pltpu.SemaphoreType.DMA
    out, top = pl.pallas_call(
        functools.partial(sweeps_kernel, nodes, quad),
        out_shape=(
            jax.ShapeDtypeStruct((cells, size_y, size_z), jnp.float32),
            jax.ShapeDtypeStruct((8, 128), jnp.float32),
        ),
        in_specs=[whole] * 5,
        out_specs=(whole, whole),
        scratch_shapes=[
            room(2, cells, size_y, size_z),
            room(chunks, node_count, total_x, rows, size_z),
            room(chunks, total_x, rows, size_z),
            room(total_x, node_count, rows, size_z),
            room(total_x, node_count, rows, size_z),
            room(chunks, SWEEPS + 1, total_x, rows, size_z),
            room(SWEEPS + 1, cells, size_y, size_z),
            room(node_count, rows, size_z),
            room(node_count, rows, size_z),
            room(node_count, rows, size_z),
            room(8, 128),
            room(slab_count, 8, 128),
            room(node_count, 8, 128),
            dma((chunks, slab_count)),
            dma((chunks, slab_count)),
            dma((chunks, slab_count)),
            dma((chunks, slab_count)),
            dma((chunks, node_count, 2)),
            dma((chunks, node_count)),
            dma((chunks, slab_count)),
            dma((chunks, slab_count)),
            dma((2, max(slab_count, node_count))),
            dma((2, max(slab_count, node_count))),
            dma((3, chunks)),
        ],
        compiler_params=pltpu.CompilerParams(
            collective_id=0, has_side_effects=True, vmem_limit_bytes=60 * 1024 * 1024
        ),
    )(sections[0], initial, lam, matrix_y, matrix_z)
    return (out[None], top[:SWEEPS, 0])


def solution(mesh):
    placed = (P("slab", None, None), P("node", "slab", None, None))
    return jax.shard_map(
        on_device,
        mesh=mesh,
        in_specs=placed,
        out_specs=(P("node", "slab", None, None), P()),
        check_vma=False,
    )
```

```python
import functools
import math

import jax
import jax.numpy as jnp
from jax import lax
from jax.experimental import pallas as pl
from jax.experimental.pallas import tpu as pltpu
from jax.sharding import PartitionSpec as P

SWEEPS = 3


diffusion_step = 4.0
MESH = pl.DeviceIdType.MESH


def radau_value(order, point):
    prev_value = 1.0
    prev_slope = 0.0
    this_value = point
    this_slope = 1.0
    for degree in range(1, order):
        next_value = ((2 * degree + 1) * point * this_value - degree * prev_value) / (degree + 1)
        next_slope = (
            (2 * degree + 1) * (this_value + point * this_slope) - degree * prev_slope
        ) / (degree + 1)
        prev_value, prev_slope = (this_value, this_slope)
        this_value, this_slope = (next_value, next_slope)
    return (this_value - prev_value, this_slope - prev_slope)


def radau_tables(node_total):
    points = []
    for node_index in range(node_total):
        estimate = math.cos(2.0 * math.pi * node_index / (2 * node_total - 1))
        if node_index > 0:
            for repeat in range(60):
                poly_value, poly_slope = radau_value(node_total, estimate)
                estimate = estimate - poly_value / poly_slope
        points.append((estimate + 1.0) / 2.0)
    points = sorted(points)
    quadrature = []
    for row_index in range(node_total):
        entries = []
        for column_index in range(node_total):
            coeffs = [1.0]
            for other_index in range(node_total):
                if other_index != column_index:
                    divisor = points[column_index] - points[other_index]
                    shifted = [0.0] + coeffs
                    widened = coeffs + [0.0]
                    coeffs = [
                        (shifted[place] - points[other_index] * widened[place]) / divisor
                        for place in range(len(shifted))
                    ]
            integral = 0.0
            for place in range(len(coeffs)):
                integral = integral + coeffs[place] * points[row_index] ** (place + 1) / (place + 1)
            entries.append(integral)
        quadrature.append(entries)
    return (points, quadrature)


def cas_table(length):
    indices = lax.iota(jnp.int32, length)
    products = indices[:, None] * indices[None, :] % length
    phases = products.astype(jnp.float32) * (2.0 * math.pi / length)
    return jnp.cos(phases) + jnp.sin(phases)


def eigen_line(length):
    indices = lax.iota(jnp.int32, length).astype(jnp.float32)
    return 2.0 * jnp.cos(indices * (2.0 * math.pi / length)) - 2.0


def split_terms(value):
    upper = value.astype(jnp.bfloat16)
    lower = (value - upper.astype(jnp.float32)).astype(jnp.bfloat16)
    return upper, lower


def table_terms(table):
    upper = lax.reduce_precision(table, 8, 7)
    return jnp.stack([upper.astype(jnp.bfloat16), (table - upper).astype(jnp.bfloat16)])


def product(left, right):
    def one(a, b):
        return jnp.dot(a, b, preferred_element_type=jnp.float32)

    return one(left[0], right[0]) + (one(left[0], right[1]) + one(left[1], right[0]))


def loop(count, step, carry, group=4):
    group = group if count % group == 0 else 1

    def body(index, state):
        for offset in range(group):
            state = step(index * group + offset, state)
        return state

    return lax.fori_loop(0, count // group, body, carry)


def sweeps_kernel(
    nodes, quad, u, first, lam, ymat_ref, zmat_ref, out, top,
    planes, gathered, start, resid, front, outward, arrived, rho, gain, close, peak, peers, lines,
    send_u, recv_u, send_i, recv_i, send_z, recv_z, send_r, recv_r, send_m, recv_m, local,
):
    node_count, slab_count = len(nodes), lax.axis_size("slab")
    me, here = lax.axis_index("node"), lax.axis_index("slab")
    cells, size_y, size_z = u.shape
    chunks, _, total_x, rows, lanes = gathered.shape
    parts = size_z // lanes
    band = chunks // parts * rows
    scale = 1.0 / float(size_y * size_z)

    def other_slab(step):
        return lax.rem(here + step, slab_count)

    def other_node(step):
        return lax.rem(me + step, node_count)

    def to(src, dst, send, recv, node, slab):
        return pltpu.make_async_remote_copy(
            src_ref=src, dst_ref=dst, send_sem=send, recv_sem=recv,
            device_id=(node, slab), device_id_type=MESH,
        )

    barrier = pltpu.get_barrier_semaphore()
    for step in range(1, slab_count):
        pl.semaphore_signal(barrier, inc=1, device_id=(me, other_slab(step)), device_id_type=MESH)
    for step in range(1, node_count):
        pl.semaphore_signal(barrier, inc=1, device_id=(other_node(step), here), device_id_type=MESH)

    def transform(value):
        part = product(split_terms(value), (zmat_ref[0], zmat_ref[1]))
        return product((ymat_ref[0], ymat_ref[1]), split_terms(part))

    def place_of(chunk, slab):
        first_row = slab * band + chunk // parts * rows
        return pl.ds(first_row, rows), pl.ds(chunk % parts * lanes, lanes)

    def source(field, chunk, slab):
        span, columns = place_of(chunk, slab)
        return planes.at[field, :, span, columns]

    def target(field, chunk, slab):
        span = pl.ds(slab * cells, cells)
        return gathered.at[chunk, me, span] if field == 0 else start.at[chunk, span]

    def send_field(field, send, recv):
        for chunk in range(chunks):
            pltpu.make_async_copy(
                source(field, chunk, here), target(field, chunk, here), local.at[field, chunk]
            ).start()
            for step in range(1, slab_count):
                slab = other_slab(step)
                to(
                    source(field, chunk, slab), target(field, chunk, here),
                    send.at[chunk, step], recv.at[chunk, step], me, slab,
                ).start()

    def take_field(field, chunk, send, recv):
        pltpu.make_async_copy(
            source(field, chunk, here), target(field, chunk, here), local.at[field, chunk]
        ).wait()
        for step in range(1, slab_count):
            slab = lax.rem(here + slab_count - step, slab_count)
            to(
                source(field, chunk, slab), target(field, chunk, slab),
                send.at[chunk, step], recv.at[chunk, step], me, slab,
            ).wait()

    def enter(index, state):
        planes[0, index] = transform(u[index])
        return state

    def enter_first(index, state):
        planes[1, index] = transform(first[index])
        return state

    lax.fori_loop(0, cells, enter, 0)
    pl.semaphore_wait(barrier, slab_count - 1 + node_count - 1)
    send_field(0, send_u, recv_u)
    lax.fori_loop(0, cells, enter_first, 0)
    send_field(1, send_i, recv_i)

    def piece(chunk, origin, direction):
        target_node = me + 1 if direction == 0 else me - 1
        slot = gathered.at[chunk, origin]
        return to(
            slot, slot, send_z.at[chunk, origin, direction], recv_z.at[chunk, origin],
            target_node, here,
        )

    has_right, has_left = me < node_count - 1, me > 0

    def launch(chunk):
        take_field(0, chunk, send_u, recv_u)

        @pl.when(has_right)
        def _():
            piece(chunk, me, 0).start()

        @pl.when(has_left)
        def _():
            piece(chunk, me, 1).start()

    def forward_on(chunk, away):
        @pl.when(jnp.logical_and(me - away >= 0, has_right))
        def _():
            piece(chunk, me - away, 0).wait_recv()
            piece(chunk, me - away, 0).start()

        @pl.when(jnp.logical_and(me + away < node_count, has_left))
        def _():
            piece(chunk, me + away, 1).wait_recv()
            piece(chunk, me + away, 1).start()

    def absorb(chunk):
        for away in range(1, node_count):

            @pl.when(jnp.logical_and(me - away >= 0, me == node_count - 1))
            def _():
                piece(chunk, me - away, 0).wait_recv()

            @pl.when(jnp.logical_and(me + away < node_count, me == 0))
            def _():
                piece(chunk, me + away, 1).wait_recv()

    def mix(table, values):
        mixed = []
        for line in table:
            total = line[0] * values[0]
            for weight, value in zip(line[1:], values[1:]):
                total = total + weight * value
            mixed.append(total)
        return mixed

    def solve(chunk):
        eigen = lam[pl.ds(chunk // parts * rows, rows), pl.ds(chunk % parts * lanes, lanes)]

        def between(stage):
            if chunk + 1 < chunks:
                for away in range(1 + stage, node_count, SWEEPS):
                    forward_on(chunk + 1, away)

        def blend(x, state):
            values = [gathered[chunk, j, x] for j in range(node_count)]
            for m, value in enumerate(mix(quad, values)):
                front[x, m] = value
            return state

        def begin(x, state):
            below = lax.rem(x + total_x - 1, total_x)
            above = lax.rem(x + 1, total_x)
            for m in range(node_count):
                slope = front[below, m] + front[above, m] + (eigen - 2.0) * front[x, m]
                resid[x, m] = start[chunk, x] + diffusion_step * slope - gathered[chunk, m, x]
            return state

        loop(total_x, blend, 0)
        loop(total_x, begin, 0)
        for sweep in range(SWEEPS):
            between(sweep)
            last = sweep + 1 == SWEEPS
            for m in range(node_count):
                reach = diffusion_step * nodes[m] / (sweep + 1.0)
                excess = 1.0 / reach - eigen
                root = jnp.sqrt(excess * (excess + 4.0))
                ratio = 2.0 / (excess + 2.0 + root)
                rho[m] = ratio
                gain[m] = 1.0 / (reach * root)
                power, base, left = None, ratio, total_x
                while left:
                    if left % 2:
                        power = base if power is None else power * base
                    base, left = base * base, left // 2
                close[m] = 1.0 / (1.0 - power)
            pick = pl.ds(me, 1) if last else pl.ds(0, node_count)
            width = 1 if last else node_count
            ratio = rho[pick]
            factor = gain[pick]

            def gather_ends(x, state):
                up, down = state
                return (resid[x, pick] + ratio * up, resid[total_x - 1 - x, pick] + ratio * down)

            zero = jnp.zeros((width, rows, lanes), jnp.float32)
            up, down = loop(total_x, gather_ends, (zero, zero))
            closing = close[pick]

            def forward(x, state):
                state = resid[x, pick] + ratio * state
                front[x, pick] = state
                outward[chunk, sweep, x] = resid[x, me]
                return state

            def backward(index, state):
                x = total_x - 1 - index
                held = resid[x, pick]
                beyond = ratio * state
                change = factor * (front[x, pick] + beyond)
                front[x, pick] = change
                if sweep == 0:
                    outward[chunk, SWEEPS, x] = front[x, me]
                else:
                    outward[chunk, SWEEPS, x] = outward[chunk, SWEEPS, x] + front[x, me]
                if not last:
                    moved = change - held
                    table = [
                        [quad[m][j] * (sweep + 1.0) / nodes[j] - (1.0 if m == j else 0.0)
                         for j in range(node_count)]
                        for m in range(node_count)
                    ]
                    for m, value in enumerate(mix(table, [moved[j] for j in range(node_count)])):
                        resid[x, m] = value
                return held + beyond

            loop(total_x, forward, up * closing)
            loop(total_x, backward, down * closing, 2)

    def back_source(chunk, slab):
        return outward.at[chunk, :, pl.ds(slab * cells, cells)]

    def back_target(chunk, slab):
        span, columns = place_of(chunk, slab)
        return arrived.at[:, :, span, columns]

    for chunk in range(min(2, chunks)):
        launch(chunk)
    for away in range(1, node_count):
        forward_on(0, away)
    for chunk in range(chunks):
        if chunk + 2 < chunks:
            launch(chunk + 2)
        absorb(chunk)
        take_field(1, chunk, send_i, recv_i)
        solve(chunk)
        pltpu.make_async_copy(
            back_source(chunk, here), back_target(chunk, here), local.at[2, chunk]
        ).start()
        for step in range(1, slab_count):
            slab = other_slab(step)
            to(
                back_source(chunk, slab), back_target(chunk, here),
                send_r.at[chunk, step], recv_r.at[chunk, step], me, slab,
            ).start()
    for chunk in range(chunks):
        pltpu.make_async_copy(
            back_source(chunk, here), back_target(chunk, here), local.at[2, chunk]
        ).wait()
        for step in range(1, slab_count):
            slab = lax.rem(here + slab_count - step, slab_count)
            to(
                back_source(chunk, slab), back_target(chunk, slab),
                send_r.at[chunk, step], recv_r.at[chunk, step], me, slab,
            ).wait()
        for origin in range(node_count):

            @pl.when(jnp.logical_and(has_right, origin <= me))
            def _():
                piece(chunk, origin, 0).wait_send()

            @pl.when(jnp.logical_and(has_left, origin >= me))
            def _():
                piece(chunk, origin, 1).wait_send()

    peak[...] = jnp.zeros_like(peak)
    for sweep in range(SWEEPS):

        def finish(index, state):
            value = jnp.abs(transform(arrived[sweep, index]))
            return jnp.maximum(state, jnp.max(value.reshape(-1, 8, size_z), axis=0))

        most = lax.fori_loop(0, cells, finish, jnp.zeros((8, size_z), jnp.float32))
        most = jnp.max(jnp.max(most, axis=1, keepdims=True), axis=0, keepdims=True) * scale
        peak[sweep : sweep + 1, :] = jnp.broadcast_to(most, (1, peak.shape[1]))

    def swap(count, slots, level, place):
        for step in range(1, count):
            to(peak, slots.at[step], send_m.at[level, step], recv_m.at[level, step], *place(step)).start()

    def settle(count, slots, level, place):
        for step in range(1, count):
            to(peak, slots.at[step], send_m.at[level, step], recv_m.at[level, step], *place(step)).wait()
        best = peak[...]
        for step in range(1, count):
            best = jnp.maximum(best, slots[step])
        return best

    def along_slab(step):
        return (me, other_slab(step))

    def along_node(step):
        return (other_node(step), here)

    def leave(index, state):
        out[index] = u[index] + scale * transform(arrived[SWEEPS, index])
        return state

    swap(slab_count, peers, 0, along_slab)
    lax.fori_loop(0, cells // 2, leave, 0)
    peak[...] = settle(slab_count, peers, 0, along_slab)
    swap(node_count, lines, 1, along_node)
    lax.fori_loop(cells // 2, cells, leave, 0)
    top[...] = settle(node_count, lines, 1, along_node)


def on_device(initial, sections):
    node_count = lax.axis_size("node")
    slab_count = lax.axis_size("slab")
    cells, size_y, size_z = initial.shape
    total_x = cells * slab_count
    nodes, quad = radau_tables(node_count)
    band = size_y // slab_count
    rows = 8
    lanes = 128
    chunks = band // rows * (size_z // lanes)
    eigen_y = lax.dynamic_slice_in_dim(
        eigen_line(size_y), lax.axis_index("slab") * band, band, 0
    )
    lam = eigen_y[:, None] + eigen_line(size_z)[None, :]
    matrix_y = table_terms(cas_table(size_y))
    matrix_z = table_terms(cas_table(size_z))
    whole = pl.BlockSpec(memory_space=pltpu.VMEM)

    def room(*shape):
        return pltpu.VMEM(shape, jnp.float32)

    dma = pltpu.SemaphoreType.DMA
    out, top = pl.pallas_call(
        functools.partial(sweeps_kernel, nodes, quad),
        out_shape=(
            jax.ShapeDtypeStruct((cells, size_y, size_z), jnp.float32),
            jax.ShapeDtypeStruct((8, 128), jnp.float32),
        ),
        in_specs=[whole] * 5,
        out_specs=(whole, whole),
        scratch_shapes=[
            room(2, cells, size_y, size_z),
            room(chunks, node_count, total_x, rows, lanes),
            room(chunks, total_x, rows, lanes),
            room(total_x, node_count, rows, lanes),
            room(total_x, node_count, rows, lanes),
            room(chunks, SWEEPS + 1, total_x, rows, lanes),
            room(SWEEPS + 1, cells, size_y, size_z),
            room(node_count, rows, lanes),
            room(node_count, rows, lanes),
            room(node_count, rows, lanes),
            room(8, 128),
            room(slab_count, 8, 128),
            room(node_count, 8, 128),
            dma((chunks, slab_count)),
            dma((chunks, slab_count)),
            dma((chunks, slab_count)),
            dma((chunks, slab_count)),
            dma((chunks, node_count, 2)),
            dma((chunks, node_count)),
            dma((chunks, slab_count)),
            dma((chunks, slab_count)),
            dma((2, max(slab_count, node_count))),
            dma((2, max(slab_count, node_count))),
            dma((3, chunks)),
        ],
        compiler_params=pltpu.CompilerParams(
            collective_id=0, has_side_effects=True, vmem_limit_bytes=60 * 1024 * 1024
        ),
    )(sections[0], initial, lam, matrix_y, matrix_z)
    return (out[None], top[:SWEEPS, 0])


def solution(mesh):
    placed = (P("slab", None, None), P("node", "slab", None, None))
    return jax.shard_map(
        on_device,
        mesh=mesh,
        in_specs=placed,
        out_specs=(P("node", "slab", None, None), P()),
        check_vma=False,
    )
```

```python
import functools
import math

import jax
import jax.numpy as jnp
import numpy as np
from jax import lax
from jax.experimental import pallas as pl
from jax.experimental.pallas import tpu as pltpu
from jax.sharding import PartitionSpec as P

SWEEPS = 3


diffusion_step = 4.0
MESH = pl.DeviceIdType.MESH


def radau_value(order, point):
    prev_value = 1.0
    prev_slope = 0.0
    this_value = point
    this_slope = 1.0
    for degree in range(1, order):
        next_value = ((2 * degree + 1) * point * this_value - degree * prev_value) / (degree + 1)
        next_slope = (
            (2 * degree + 1) * (this_value + point * this_slope) - degree * prev_slope
        ) / (degree + 1)
        prev_value, prev_slope = (this_value, this_slope)
        this_value, this_slope = (next_value, next_slope)
    return (this_value - prev_value, this_slope - prev_slope)


def radau_tables(node_total):
    points = []
    for node_index in range(node_total):
        estimate = math.cos(2.0 * math.pi * node_index / (2 * node_total - 1))
        if node_index > 0:
            for repeat in range(60):
                poly_value, poly_slope = radau_value(node_total, estimate)
                estimate = estimate - poly_value / poly_slope
        points.append((estimate + 1.0) / 2.0)
    points = sorted(points)
    quadrature = []
    for row_index in range(node_total):
        entries = []
        for column_index in range(node_total):
            coeffs = [1.0]
            for other_index in range(node_total):
                if other_index != column_index:
                    divisor = points[column_index] - points[other_index]
                    shifted = [0.0] + coeffs
                    widened = coeffs + [0.0]
                    coeffs = [
                        (shifted[place] - points[other_index] * widened[place]) / divisor
                        for place in range(len(shifted))
                    ]
            integral = 0.0
            for place in range(len(coeffs)):
                integral = integral + coeffs[place] * points[row_index] ** (place + 1) / (place + 1)
            entries.append(integral)
        quadrature.append(entries)
    return (points, quadrature)


def cas_table(length):
    indices = np.arange(length)
    phases = (indices[:, None] * indices[None, :] % length) * (2.0 * math.pi / length)
    return (np.cos(phases) + np.sin(phases)).astype(np.float32)


def eigen_line(length):
    indices = lax.iota(jnp.int32, length).astype(jnp.float32)
    return 2.0 * jnp.cos(indices * (2.0 * math.pi / length)) - 2.0


def split_terms(value):
    upper = value.astype(jnp.bfloat16)
    lower = (value - upper.astype(jnp.float32)).astype(jnp.bfloat16)
    return upper, lower


def table_terms(table):
    upper = table.astype(jnp.bfloat16)
    lower = (table - upper.astype(np.float32)).astype(jnp.bfloat16)
    return jnp.asarray(np.stack([upper, lower]))


def product(left, right):
    def one(a, b):
        return jnp.dot(a, b, preferred_element_type=jnp.float32)

    return one(left[0], right[0]) + (one(left[0], right[1]) + one(left[1], right[0]))


def loop(count, step, carry, group=4):
    group = group if count % group == 0 else 1

    def body(index, state):
        for offset in range(group):
            state = step(index * group + offset, state)
        return state

    return lax.fori_loop(0, count // group, body, carry)


def sweeps_kernel(
    nodes, quad, u, first, lam, ymat_ref, zmat_ref, out, top,
    planes, gathered, start, resid, front, outward, arrived, rho, gain, close, peak, peers, lines,
    send_u, recv_u, send_i, recv_i, send_z, recv_z, send_r, recv_r, send_m, recv_m, local,
):
    node_count, slab_count = len(nodes), lax.axis_size("slab")
    me, here = lax.axis_index("node"), lax.axis_index("slab")
    cells, size_y, size_z = u.shape
    chunks, _, total_x, rows, lanes = gathered.shape
    parts = size_z // lanes
    band = chunks // parts * rows
    scale = 1.0 / float(size_y * size_z)

    def other_slab(step):
        return lax.rem(here + step, slab_count)

    def other_node(step):
        return lax.rem(me + step, node_count)

    def to(src, dst, send, recv, node, slab):
        return pltpu.make_async_remote_copy(
            src_ref=src, dst_ref=dst, send_sem=send, recv_sem=recv,
            device_id=(node, slab), device_id_type=MESH,
        )

    barrier = pltpu.get_barrier_semaphore()
    for step in range(1, slab_count):
        pl.semaphore_signal(barrier, inc=1, device_id=(me, other_slab(step)), device_id_type=MESH)
    for step in range(1, node_count):
        pl.semaphore_signal(barrier, inc=1, device_id=(other_node(step), here), device_id_type=MESH)

    def transform(value):
        part = product(split_terms(value), (zmat_ref[0], zmat_ref[1]))
        return product((ymat_ref[0], ymat_ref[1]), split_terms(part))

    def place_of(chunk, slab):
        first_row = slab * band + chunk // parts * rows
        return pl.ds(first_row, rows), pl.ds(chunk % parts * lanes, lanes)

    def source(field, chunk, slab):
        span, columns = place_of(chunk, slab)
        return planes.at[field, :, span, columns]

    def target(field, chunk, slab):
        span = pl.ds(slab * cells, cells)
        return gathered.at[chunk, me, span] if field == 0 else start.at[chunk, span]

    def send_field(field, send, recv):
        for chunk in range(chunks):
            pltpu.make_async_copy(
                source(field, chunk, here), target(field, chunk, here), local.at[field, chunk]
            ).start()
            for step in range(1, slab_count):
                slab = other_slab(step)
                to(
                    source(field, chunk, slab), target(field, chunk, here),
                    send.at[chunk, step], recv.at[chunk, step], me, slab,
                ).start()

    def take_field(field, chunk, send, recv):
        pltpu.make_async_copy(
            source(field, chunk, here), target(field, chunk, here), local.at[field, chunk]
        ).wait()
        for step in range(1, slab_count):
            slab = lax.rem(here + slab_count - step, slab_count)
            to(
                source(field, chunk, slab), target(field, chunk, slab),
                send.at[chunk, step], recv.at[chunk, step], me, slab,
            ).wait()

    def enter(index, state):
        planes[0, index] = transform(u[index])
        return state

    def enter_first(index, state):
        planes[1, index] = transform(first[index])
        return state

    lax.fori_loop(0, cells, enter, 0)
    pl.semaphore_wait(barrier, slab_count - 1 + node_count - 1)
    send_field(0, send_u, recv_u)
    lax.fori_loop(0, cells, enter_first, 0)
    send_field(1, send_i, recv_i)

    def piece(chunk, origin, direction):
        target_node = me + 1 if direction == 0 else me - 1
        slot = gathered.at[chunk, origin]
        return to(
            slot, slot, send_z.at[chunk, origin, direction], recv_z.at[chunk, origin],
            target_node, here,
        )

    has_right, has_left = me < node_count - 1, me > 0

    def launch(chunk):
        take_field(0, chunk, send_u, recv_u)

        @pl.when(has_right)
        def _():
            piece(chunk, me, 0).start()

        @pl.when(has_left)
        def _():
            piece(chunk, me, 1).start()

    def forward_on(chunk, away):
        @pl.when(jnp.logical_and(me - away >= 0, has_right))
        def _():
            piece(chunk, me - away, 0).wait_recv()
            piece(chunk, me - away, 0).start()

        @pl.when(jnp.logical_and(me + away < node_count, has_left))
        def _():
            piece(chunk, me + away, 1).wait_recv()
            piece(chunk, me + away, 1).start()

    def absorb(chunk):
        for away in range(1, node_count):

            @pl.when(jnp.logical_and(me - away >= 0, me == node_count - 1))
            def _():
                piece(chunk, me - away, 0).wait_recv()

            @pl.when(jnp.logical_and(me + away < node_count, me == 0))
            def _():
                piece(chunk, me + away, 1).wait_recv()

    def mix(table, values):
        mixed = []
        for line in table:
            total = line[0] * values[0]
            for weight, value in zip(line[1:], values[1:]):
                total = total + weight * value
            mixed.append(total)
        return mixed

    def solve(chunk):
        eigen = lam[pl.ds(chunk // parts * rows, rows), pl.ds(chunk % parts * lanes, lanes)]

        def between(stage):
            if chunk + 1 < chunks:
                for away in range(1 + stage, node_count, SWEEPS):
                    forward_on(chunk + 1, away)

        def blend(x, state):
            values = [gathered[chunk, j, x] for j in range(node_count)]
            for m, value in enumerate(mix(quad, values)):
                front[x, m] = value
            return state

        def begin(x, state):
            below = lax.rem(x + total_x - 1, total_x)
            above = lax.rem(x + 1, total_x)
            for m in range(node_count):
                slope = front[below, m] + front[above, m] + (eigen - 2.0) * front[x, m]
                resid[x, m] = start[chunk, x] + diffusion_step * slope - gathered[chunk, m, x]
            return state

        loop(total_x, blend, 0)
        loop(total_x, begin, 0)
        for sweep in range(SWEEPS):
            between(sweep)
            last = sweep + 1 == SWEEPS
            for m in range(node_count):
                reach = diffusion_step * nodes[m] / (sweep + 1.0)
                excess = 1.0 / reach - eigen
                root = jnp.sqrt(excess * (excess + 4.0))
                ratio = 2.0 / (excess + 2.0 + root)
                rho[m] = ratio
                gain[m] = 1.0 / (reach * root)
                power, base, left = None, ratio, total_x
                while left:
                    if left % 2:
                        power = base if power is None else power * base
                    base, left = base * base, left // 2
                close[m] = 1.0 / (1.0 - power)
            pick = pl.ds(me, 1) if last else pl.ds(0, node_count)
            width = 1 if last else node_count
            ratio = rho[pick]
            factor = gain[pick]

            def gather_ends(x, state):
                up, down = state
                return (resid[x, pick] + ratio * up, resid[total_x - 1 - x, pick] + ratio * down)

            zero = jnp.zeros((width, rows, lanes), jnp.float32)
            up, down = loop(total_x, gather_ends, (zero, zero))
            closing = close[pick]

            def forward(x, state):
                state = resid[x, pick] + ratio * state
                front[x, pick] = state
                outward[chunk, sweep, x] = resid[x, me]
                return state

            def backward(index, state):
                x = total_x - 1 - index
                held = resid[x, pick]
                beyond = ratio * state
                change = factor * (front[x, pick] + beyond)
                front[x, pick] = change
                if sweep == 0:
                    outward[chunk, SWEEPS, x] = front[x, me]
                else:
                    outward[chunk, SWEEPS, x] = outward[chunk, SWEEPS, x] + front[x, me]
                if not last:
                    moved = change - held
                    table = [
                        [quad[m][j] * (sweep + 1.0) / nodes[j] - (1.0 if m == j else 0.0)
                         for j in range(node_count)]
                        for m in range(node_count)
                    ]
                    for m, value in enumerate(mix(table, [moved[j] for j in range(node_count)])):
                        resid[x, m] = value
                return held + beyond

            loop(total_x, forward, up * closing)
            loop(total_x, backward, down * closing, 2)

    def back_source(chunk, slab):
        return outward.at[chunk, :, pl.ds(slab * cells, cells)]

    def back_target(chunk, slab):
        span, columns = place_of(chunk, slab)
        return arrived.at[:, :, span, columns]

    for chunk in range(min(2, chunks)):
        launch(chunk)
    for away in range(1, node_count):
        forward_on(0, away)
    for chunk in range(chunks):
        if chunk + 2 < chunks:
            launch(chunk + 2)
        absorb(chunk)
        take_field(1, chunk, send_i, recv_i)
        solve(chunk)
        pltpu.make_async_copy(
            back_source(chunk, here), back_target(chunk, here), local.at[2, chunk]
        ).start()
        for step in range(1, slab_count):
            slab = other_slab(step)
            to(
                back_source(chunk, slab), back_target(chunk, here),
                send_r.at[chunk, step], recv_r.at[chunk, step], me, slab,
            ).start()
    for chunk in range(chunks):
        pltpu.make_async_copy(
            back_source(chunk, here), back_target(chunk, here), local.at[2, chunk]
        ).wait()
        for step in range(1, slab_count):
            slab = lax.rem(here + slab_count - step, slab_count)
            to(
                back_source(chunk, slab), back_target(chunk, slab),
                send_r.at[chunk, step], recv_r.at[chunk, step], me, slab,
            ).wait()
        for origin in range(node_count):

            @pl.when(jnp.logical_and(has_right, origin <= me))
            def _():
                piece(chunk, origin, 0).wait_send()

            @pl.when(jnp.logical_and(has_left, origin >= me))
            def _():
                piece(chunk, origin, 1).wait_send()

    peak[...] = jnp.zeros_like(peak)
    for sweep in range(SWEEPS):

        def finish(index, state):
            value = jnp.abs(transform(arrived[sweep, index]))
            return jnp.maximum(state, jnp.max(value.reshape(-1, 8, size_z), axis=0))

        most = lax.fori_loop(0, cells, finish, jnp.zeros((8, size_z), jnp.float32))
        most = jnp.max(jnp.max(most, axis=1, keepdims=True), axis=0, keepdims=True) * scale
        peak[sweep : sweep + 1, :] = jnp.broadcast_to(most, (1, peak.shape[1]))

    def swap(count, slots, level, place):
        for step in range(1, count):
            to(peak, slots.at[step], send_m.at[level, step], recv_m.at[level, step], *place(step)).start()

    def settle(count, slots, level, place):
        for step in range(1, count):
            to(peak, slots.at[step], send_m.at[level, step], recv_m.at[level, step], *place(step)).wait()
        best = peak[...]
        for step in range(1, count):
            best = jnp.maximum(best, slots[step])
        return best

    def along_slab(step):
        return (me, other_slab(step))

    def along_node(step):
        return (other_node(step), here)

    def leave(index, state):
        out[index] = u[index] + scale * transform(arrived[SWEEPS, index])
        return state

    swap(slab_count, peers, 0, along_slab)
    lax.fori_loop(0, cells // 2, leave, 0)
    peak[...] = settle(slab_count, peers, 0, along_slab)
    swap(node_count, lines, 1, along_node)
    lax.fori_loop(cells // 2, cells, leave, 0)
    top[...] = settle(node_count, lines, 1, along_node)


def on_device(initial, sections):
    node_count = lax.axis_size("node")
    slab_count = lax.axis_size("slab")
    cells, size_y, size_z = initial.shape
    total_x = cells * slab_count
    nodes, quad = radau_tables(node_count)
    band = size_y // slab_count
    rows = 8
    lanes = 128
    chunks = band // rows * (size_z // lanes)
    eigen_y = lax.dynamic_slice_in_dim(
        eigen_line(size_y), lax.axis_index("slab") * band, band, 0
    )
    lam = eigen_y[:, None] + eigen_line(size_z)[None, :]
    matrix_y = table_terms(cas_table(size_y))
    matrix_z = table_terms(cas_table(size_z))
    whole = pl.BlockSpec(memory_space=pltpu.VMEM)

    def room(*shape):
        return pltpu.VMEM(shape, jnp.float32)

    dma = pltpu.SemaphoreType.DMA
    out, top = pl.pallas_call(
        functools.partial(sweeps_kernel, nodes, quad),
        out_shape=(
            jax.ShapeDtypeStruct((cells, size_y, size_z), jnp.float32),
            jax.ShapeDtypeStruct((8, 128), jnp.float32),
        ),
        in_specs=[whole] * 5,
        out_specs=(whole, whole),
        scratch_shapes=[
            room(2, cells, size_y, size_z),
            room(chunks, node_count, total_x, rows, lanes),
            room(chunks, total_x, rows, lanes),
            room(total_x, node_count, rows, lanes),
            room(total_x, node_count, rows, lanes),
            room(chunks, SWEEPS + 1, total_x, rows, lanes),
            room(SWEEPS + 1, cells, size_y, size_z),
            room(node_count, rows, lanes),
            room(node_count, rows, lanes),
            room(node_count, rows, lanes),
            room(8, 128),
            room(slab_count, 8, 128),
            room(node_count, 8, 128),
            dma((chunks, slab_count)),
            dma((chunks, slab_count)),
            dma((chunks, slab_count)),
            dma((chunks, slab_count)),
            dma((chunks, node_count, 2)),
            dma((chunks, node_count)),
            dma((chunks, slab_count)),
            dma((chunks, slab_count)),
            dma((2, max(slab_count, node_count))),
            dma((2, max(slab_count, node_count))),
            dma((3, chunks)),
        ],
        compiler_params=pltpu.CompilerParams(
            collective_id=0, has_side_effects=True, vmem_limit_bytes=60 * 1024 * 1024
        ),
    )(sections[0], initial, lam, matrix_y, matrix_z)
    return (out[None], top[:SWEEPS, 0])


def solution(mesh):
    placed = (P("slab", None, None), P("node", "slab", None, None))
    return jax.shard_map(
        on_device,
        mesh=mesh,
        in_specs=placed,
        out_specs=(P("node", "slab", None, None), P()),
        check_vma=False,
    )
```
